8 devices in a mesh: mp: 2 (over z, y), fsdp: 4 (over x, core).
Axes of the slice: x: 2, y: 2, z: 1, core: 2. Of those that a mesh axis runs over, the one named last changes fastest.
Arguments:
- x: bfloat16 [1, 8, 4096, 1536], P(None, ('mp', 'fsdp')), parts along dimension 1
- dy: bfloat16 [8, 4096, 1536], P(('mp', 'fsdp')), parts along dimension 0
- xn: bfloat16 [8, 4096, 1536], P(('mp', 'fsdp')), parts along dimension 0
- w1: float32 [1, 3072, 6144], P(None, ('mp', 'fsdp')), parts along dimension 1
- w2: float32 [1, 12288, 1536], P(None, ('mp', 'fsdp')), parts along dimension 1
- g1: float32 [1, 3072, 6144], P(None, ('mp', 'fsdp')), parts along dimension 1
- g2: float32 [1, 12288, 1536], P(None, ('mp', 'fsdp')), parts along dimension 1
- m1: float32 [1, 3072, 6144], P(None, ('mp', 'fsdp')), parts along dimension 1
- m2: float32 [1, 12288, 1536], P(None, ('mp', 'fsdp')), parts along dimension 1
- v1: float32 [1, 3072, 6144], P(None, ('mp', 'fsdp')), parts along dimension 1
- v2: float32 [1, 12288, 1536], P(None, ('mp', 'fsdp')), parts along dimension 1
- hp: float32 [5], replicated
- step: int32 [1], replicated
Outputs:
- output 1: float32 [1, 3072, 6144], P(None, ('mp', 'fsdp')), parts along dimension 1
- output 2: float32 [1, 12288, 1536], P(None, ('mp', 'fsdp')), parts along dimension 1
- output 3: float32 [1, 3072, 6144], P(None, ('mp', 'fsdp')), parts along dimension 1
- output 4: float32 [1, 12288, 1536], P(None, ('mp', 'fsdp')), parts along dimension 1
- output 5: float32 [1, 3072, 6144], P(None, ('mp', 'fsdp')), parts along dimension 1
- output 6: float32 [1, 12288, 1536], P(None, ('mp', 'fsdp')), parts along dimension 1
- output 7: bfloat16 [8, 4096, 1536], P(('mp', 'fsdp')), parts along dimension 0
There are 2 independent parts. The reference program is written for one: setup_inputs(seed, part) draws one part's arguments, and reference() takes and returns one part's arrays. A program takes and returns all parts, laid end to end along the dimension named above; an argument that names none is the same for every part.
All inputs are finite; a program needn't handle non-finite values.
Results may differ from the reference program's by a relative error of at most 0.00473703.
Values are sent between devices in bfloat16 or wider.
A program may use at most 1 GiB of HBM per device.

```python
import jax
import jax.numpy as jnp
from jax import lax

D = 1536
FF = 6144
LAYERS = 1
BATCH_DEV = 1
SEQ = 4096
FSDP = 4


def gelu(h):
    return jax.nn.gelu(h, approximate=True)


def setup_inputs(seed: int = 0, part: int = 0) -> dict:
    kp = jax.random.fold_in(jax.random.key(seed), part)
    ks = jax.random.split(kp, 11)
    kc = jax.random.split(jax.random.key(seed + 1), 2)
    f32 = jnp.float32
    bf = jnp.bfloat16
    nb = FSDP * BATCH_DEV
    ntot = nb * SEQ
    u = jax.random.uniform(kc[0], (5,), f32)
    lr = (0.15 + 0.15 * u[0]) * D ** -0.5
    b1 = 0.85 + 0.07 * u[1]
    b2 = 0.95 + 0.04 * u[2]
    eps = 1e-8 * (1.0 + u[3])
    wd = 0.05 + 0.1 * u[4]
    hp = jnp.stack([lr, b1, b2, eps, wd]).astype(f32)
    step = jax.random.randint(kc[1], (1,), 2, 6, jnp.int32)
    tp = (step[0] - 1).astype(f32)
    c1 = 1.0 - b1 ** tp
    c2 = 1.0 - b2 ** tp
    gs1 = 0.35
    gs2 = 0.65
    s1 = (LAYERS, D, FF)
    s2 = (LAYERS, FF, D)
    return {
        'x': jax.random.normal(ks[0], (LAYERS, nb, SEQ, D), f32).astype(bf),
        'dy': (jax.random.normal(ks[1], (nb, SEQ, D), f32) * ntot ** -0.5).astype(bf),
        'xn': jax.random.normal(ks[2], (nb, SEQ, D), f32).astype(bf),
        'w1': jax.random.normal(ks[3], s1, f32) * D ** -0.5,
        'w2': jax.random.normal(ks[4], s2, f32) * FF ** -0.5,
        'g1': gs1 * jax.random.normal(ks[5], s1, f32),
        'g2': gs2 * jax.random.normal(ks[6], s2, f32),
        'm1': c1 * gs1 * jax.random.normal(ks[7], s1, f32),
        'm2': c1 * gs2 * jax.random.normal(ks[8], s2, f32),
        'v1': c2 * gs1 * gs1 * jax.random.uniform(ks[9], s1, f32, 0.5, 1.5),
        'v2': c2 * gs2 * gs2 * jax.random.uniform(ks[10], s2, f32, 0.5, 1.5),
        'hp': hp,
        'step': step,
    }


def reference(x, dy, xn, w1, w2, g1, g2, m1, m2, v1, v2, hp, step):
    f32 = jnp.float32
    bf = jnp.bfloat16
    nd = BATCH_DEV * SEQ
    wb1 = w1.astype(bf)
    wb2 = w2.astype(bf)
    xs = jnp.transpose(x.reshape(LAYERS, FSDP, nd, D), (1, 0, 2, 3))
    dys = dy.reshape(FSDP, nd, D)

    def one_device(carry, inp):
        xd, gy = inp
        acc1, acc2 = carry
        p1 = [None] * LAYERS
        p2 = [None] * LAYERS
        for l in reversed(range(LAYERS)):
            xl = xd[l]
            h = jnp.dot(xl, wb1[l], preferred_element_type=f32)
            a, gv = jax.vjp(gelu, h)
            a = a.astype(bf)
            da = jnp.dot(gy, wb2[l].T, preferred_element_type=f32)
            dh = gv(da)[0].astype(bf)
            p2[l] = jnp.dot(a.T, gy, preferred_element_type=f32).astype(bf)
            p1[l] = jnp.dot(xl.T, dh, preferred_element_type=f32).astype(bf)
            if l > 0:
                gy = (gy.astype(f32) + jnp.dot(dh, wb1[l].T, preferred_element_type=f32)).astype(bf)
        acc1 = acc1 + jnp.stack(p1).astype(f32)
        acc2 = acc2 + jnp.stack(p2).astype(f32)
        return (acc1, acc2), None

    init = (jnp.zeros((LAYERS, D, FF), f32), jnp.zeros((LAYERS, FF, D), f32))
    (s1, s2), _ = lax.scan(one_device, init, (xs, dys))
    tf = step[0].astype(f32)
    lr, b1, b2, eps, wd = hp[0], hp[1], hp[2], hp[3], hp[4]

    def adam(w, ga, s, m, v):
        g = (ga + s) / 2.0
        mn = b1 * m + (1.0 - b1) * g
        vn = b2 * v + (1.0 - b2) * g * g
        upd = (mn / (1.0 - b1 ** tf)) / (jnp.sqrt(vn / (1.0 - b2 ** tf)) + eps)
        return w - lr * (upd + wd * w), mn, vn

    nw1, nm1, nv1 = adam(w1, g1, s1, m1, v1)
    nw2, nm2, nv2 = adam(w2, g2, s2, m2, v2)
    nb1 = nw1.astype(bf)
    nb2 = nw2.astype(bf)

    def fwd(xc):
        for l in range(LAYERS):
            h = jnp.dot(xc, nb1[l], preferred_element_type=f32)
            a = gelu(h).astype(bf)
            xc = (xc.astype(f32) + jnp.dot(a, nb2[l], preferred_element_type=f32)).astype(bf)
        return xc

    xo = lax.map(fwd, xn.reshape(FSDP, nd, D)).reshape(FSDP * BATCH_DEV, SEQ, D)
    return (nw1, nw2, nm1, nm2, nv1, nv2, xo)
```

```python
import jax
import jax.numpy as jnp
from jax import lax
from jax.sharding import PartitionSpec as P

NK = 2


def gelu(h):
    return jax.nn.gelu(h, approximate=True)


def adam(w, ga, s, m, v, hp, tf):
    lr, b1, b2, eps, wd = hp[0], hp[1], hp[2], hp[3], hp[4]
    g = (ga + s) / 2.0
    mn = b1 * m + (1.0 - b1) * g
    vn = b2 * v + (1.0 - b2) * g * g
    upd = (mn / (1.0 - b1 ** tf)) / (jnp.sqrt(vn / (1.0 - b2 ** tf)) + eps)
    return w - lr * (upd + wd * w), mn, vn


def solution(mesh):
    n = mesh.shape['fsdp']
    f32 = jnp.float32
    bf = jnp.bfloat16
    tok4 = P(None, ('mp', 'fsdp'), None, None)
    tok3 = P(('mp', 'fsdp'), None, None)
    rows = P(None, ('mp', 'fsdp'), None)

    def gather(c):
        return lax.all_gather(c, 'fsdp', axis=0, tiled=True)

    def body(x, dy, xn, w1, w2, g1, g2, m1, m2, v1, v2, hp, step):
        _, b, t, d = x.shape
        ds = w1.shape[1]
        ff = w1.shape[2]
        fs = w2.shape[1]
        fk = fs // NK
        tf = step[0].astype(f32)
        me = lax.axis_index('fsdp')
        gy = dy.reshape(b * t, d)
        xl = x.reshape(b * t, d)
        xc = xn.reshape(b * t, d)

        def cols(c, k):
            return c.reshape(ds, n, NK, fk)[:, :, k].reshape(ds, n * fk)

        c1s = w1[0].astype(bf)
        c2s = w2[0].astype(bf)
        got1 = []
        got2 = []
        for k in range(NK):
            got1.append(gather(cols(c1s, k)))
            got2.append(gather(c2s[k * fk:(k + 1) * fk]))
        r1 = [[None] * NK for _ in range(n)]
        r2 = [[None] * NK for _ in range(n)]
        for k in range(NK):
            h = jnp.dot(xl, got1[k], preferred_element_type=f32)
            a, gv = jax.vjp(gelu, h)
            a = a.astype(bf)
            p2 = jnp.einsum('nf,nd->fd', a, gy, preferred_element_type=f32).astype(bf)
            for r in range(n):
                q = lax.dynamic_slice_in_dim(p2, (me ^ r) * fk, fk, 0)
                r2[r][k] = q if r == 0 else lax.ppermute(q, 'fsdp', [(i, i ^ r) for i in range(n)])
            da = jnp.einsum('nd,fd->nf', gy, got2[k], preferred_element_type=f32)
            dh = gv(da)[0].astype(bf)
            p1 = jnp.einsum('nd,nf->df', xl, dh, preferred_element_type=f32).astype(bf)
            for r in range(n):
                q = lax.dynamic_slice_in_dim(p1, (me ^ r) * ds, ds, 0)
                r1[r][k] = q if r == 0 else lax.ppermute(q, 'fsdp', [(i, i ^ r) for i in range(n)])

        s1 = 0.0
        s2 = 0.0
        for r in range(n):
            s1 = s1 + jnp.stack([q.reshape(ds, n, fk) for q in r1[r]], axis=2).reshape(ds, ff).astype(f32)
            s2 = s2 + jnp.concatenate(r2[r], axis=0).astype(f32)
        w1n, m1n, v1n = adam(w1[0], g1[0], s1, m1[0], v1[0], hp, tf)
        w2n, m2n, v2n = adam(w2[0], g2[0], s2, m2[0], v2[0], hp, tf)
        c1n = w1n.astype(bf)
        c2n = w2n.astype(bf)
        out = xc.astype(f32)
        for k in range(NK):
            h = jnp.dot(xc, gather(cols(c1n, k)), preferred_element_type=f32)
            a = gelu(h).astype(bf)
            out = out + jnp.dot(a, gather(c2n[k * fk:(k + 1) * fk]), preferred_element_type=f32)
        return (w1n[None], w2n[None], m1n[None], m2n[None], v1n[None], v2n[None],
                out.astype(bf).reshape(b, t, d))

    return jax.shard_map(body, mesh=mesh,
                         in_specs=(tok4, tok3, tok3) + (rows,) * 8 + (P(), P()),
                         out_specs=(rows,) * 6 + (tok3,), check_vma=False)
```

```python
import functools

import jax
import jax.numpy as jnp
from jax import lax
from jax.experimental import pallas as pl
from jax.experimental.pallas import tpu as pltpu
from jax.sharding import PartitionSpec as P


NK = 4
TM = 512
TN = 512
C0 = 0.7978845608028654
C1 = 0.044715
f32 = jnp.float32
bf = jnp.bfloat16
VMEM = 60 * 1024 * 1024
LATER = pl.BlockSpec(memory_space=pl.ANY)


def params(n=1):
    return pltpu.CompilerParams(vmem_limit_bytes=VMEM, dimension_semantics=("arbitrary",) * n)


def whole(shape, row=0):
    return pl.BlockSpec(shape, lambda *_: (row, 0), pipeline_mode=pl.Buffered(1))


def cost(flops, nbytes):
    return pl.CostEstimate(flops=flops, bytes_accessed=nbytes, transcendentals=0)


def cast_kernel(w1, w2, out):
    r = w1.shape[0]
    out[:r] = w1[...].astype(bf)
    out[r:] = w2[...].astype(bf)


def cast_chunk(w1, w2, k, n):
    r, cb = w1.shape[0], w1.shape[1] // (n * NK)
    d = w2.shape[1]
    rb, dc = w2.shape[0] // NK, d // n
    return pl.pallas_call(
        cast_kernel, grid=(n,),
        in_specs=[pl.BlockSpec((r, cb), lambda j: (0, j * NK + k)),
                  pl.BlockSpec((rb, dc), lambda j: (k, j))],
        out_specs=pl.BlockSpec((r + rb, cb), lambda j: (0, j)),
        out_shape=jax.ShapeDtypeStruct((r + rb, d), bf),
        cost_estimate=cost(r * d * 2, r * d * 12),
        name="cast_chunk", compiler_params=params())(w1, w2)


def join1(me, cs, n, w1):
    b = cs[0].shape[0]
    w = w1.shape[1] // n
    for q in range(n):
        for r in range(n):
            j = pl.multiple_of((me ^ r) * w, 128)
            w1[pl.ds(pl.multiple_of((me ^ q) * b, 128), b), r * w:(r + 1) * w] = cs[q][:, pl.ds(j, w)]


def join2(cs, n, w2):
    b = cs[0].shape[0]
    for q in range(n):
        w2[q * b:(q + 1) * b, :] = cs[q][...]


def hid_kernel(n, me, x, dy, *refs):
    c1, c2 = refs[:n], refs[n:2 * n]
    a_out, dh_out, w1, w2 = refs[-4:]

    @pl.when(pl.program_id(0) == 0)
    def _():
        join1(me[0], c1, n, w1)
        join2(c2, n, w2)

    xv = x[...]
    dv = dy[...]
    for s in range(0, w1.shape[1], TN):
        h = jnp.dot(xv, w1[:, s:s + TN], preferred_element_type=f32)
        da = lax.dot_general(dv, w2[s:s + TN, :], (((1,), (1,)), ((), ())),
                             preferred_element_type=f32)
        hh = h * h
        t = jnp.tanh(h * (C0 + (C0 * C1) * hh))
        p = 0.5 + 0.5 * t
        a_out[:, s:s + TN] = (h * p).astype(bf)
        gp = p + (0.5 * h) * (1.0 - t * t) * (C0 + (3.0 * C0 * C1) * hh)
        dh_out[:, s:s + TN] = (da * gp).astype(bf)


def hid(me, x, dy, cs, after):
    n = len(cs)
    t, d = x.shape
    h2, w = cs[0].shape
    hh = h2 // 2
    tok = pl.BlockSpec((TM, d), lambda i, *_: (i, 0))
    return pl.pallas_call(
        functools.partial(hid_kernel, n),
        grid_spec=pltpu.PrefetchScalarGridSpec(
            num_scalar_prefetch=1, grid=(t // TM,),
            in_specs=[tok, tok] + [whole((hh, w))] * n + [whole((hh, w), 1)] * n + [LATER] * len(after),
            out_specs=[pl.BlockSpec((TM, w), lambda i, *_: (i, 0))] * 2,
            scratch_shapes=[pltpu.VMEM((n * hh, w), bf), pltpu.VMEM((n * hh, d), bf)]),
        out_shape=[jax.ShapeDtypeStruct((t, w), bf)] * 2,
        cost_estimate=cost(4 * t * d * w, 8 * t * d),
        name="hid", compiler_params=params())(me, x, dy, *cs, *cs, *after)


def up_kernel(n, me, x, *refs):
    c1 = refs[:n]
    a_out, w1 = refs[-2:]

    @pl.when(pl.program_id(0) == 0)
    def _():
        join1(me[0], c1, n, w1)

    xv = x[...]
    for s in range(0, w1.shape[1], TN):
        h = jnp.dot(xv, w1[:, s:s + TN], preferred_element_type=f32)
        t = jnp.tanh(h * (C0 + (C0 * C1) * (h * h)))
        a_out[:, s:s + TN] = (h * (0.5 + 0.5 * t)).astype(bf)


def up(me, x, cs, after):
    n = len(cs)
    t, d = x.shape
    h2, w = cs[0].shape
    hh = h2 // 2
    return pl.pallas_call(
        functools.partial(up_kernel, n),
        grid_spec=pltpu.PrefetchScalarGridSpec(
            num_scalar_prefetch=1, grid=(t // TM,),
            in_specs=[pl.BlockSpec((TM, d), lambda i, *_: (i, 0))] + [whole((hh, w))] * n
            + [LATER] * len(after),
            out_specs=pl.BlockSpec((TM, w), lambda i, *_: (i, 0)),
            scratch_shapes=[pltpu.VMEM((n * hh, w), bf)]),
        out_shape=jax.ShapeDtypeStruct((t, w), bf),
        cost_estimate=cost(2 * t * d * w, 4 * t * d),
        name="up", compiler_params=params())(me, x, *cs, *after)


def down_kernel(n, a, acc, *refs):
    c2 = refs[:n]
    out, w2 = refs[n:]

    @pl.when(pl.program_id(0) == 0)
    def _():
        join2(c2, n, w2)

    av = a[...]
    for s in range(0, w2.shape[1], TN):
        o = jnp.dot(av, w2[:, s:s + TN], preferred_element_type=f32)
        out[:, s:s + TN] = (acc[:, s:s + TN].astype(f32) + o).astype(out.dtype)


def down(a, acc, cs, dtype):
    n = len(cs)
    t, w = a.shape
    h2, d = cs[0].shape
    hh = h2 // 2
    tok = pl.BlockSpec((TM, d), lambda i: (i, 0))
    return pl.pallas_call(
        functools.partial(down_kernel, n), grid=(t // TM,),
        in_specs=[pl.BlockSpec((TM, w), lambda i: (i, 0)), tok] + [whole((hh, d), 1)] * n,
        out_specs=tok,
        scratch_shapes=[pltpu.VMEM((n * hh, d), bf)],
        out_shape=jax.ShapeDtypeStruct((t, d), dtype),
        cost_estimate=cost(2 * t * d * w, 10 * t * d),
        name="down", compiler_params=params())(a, acc, *cs)


def adam_kernel(n, me, sc, *refs):
    lr, b1, b2, eps, wd, u1, u2 = (sc[i] for i in range(7))
    p1, p2 = refs[:n], refs[n:2 * n]
    wi = refs[2 * n:2 * n + 8]
    outs = refs[-7:]
    b = outs[6].shape[0] // 2
    for half, ps in ((0, p1), (1, p2)):
        w, ga, m, v = (wi[half * 4 + i][...] for i in range(4))
        s = ps[0][...].astype(f32)
        for q in range(1, n):
            s = s + ps[q][...].astype(f32)
        g = (ga + s) / 2.0
        mn = b1 * m + (1.0 - b1) * g
        vn = b2 * v + (1.0 - b2) * g * g
        upd = (mn / u1) / (jnp.sqrt(vn / u2) + eps)
        wn = w - lr * (upd + wd * w)
        outs[half * 3][...] = wn
        outs[half * 3 + 1][...] = mn
        outs[half * 3 + 2][...] = vn
        outs[6][half * b:(half + 1) * b, :] = wn.astype(bf)


def adam(me, sc, p1, got1, p2, got2, st1, st2, prev, k, after):
    n = len(got1) + 1
    r, ff = st1[0].shape
    f, d = st2[0].shape
    cb, rb, dc = ff // (n * NK), f // NK, d // n

    def col(q):
        return pl.BlockSpec((r, cb), lambda j, me, sc: (0 if q else me[0], me[0] ^ q ^ j))

    def straight():
        return pl.BlockSpec((rb, dc), lambda j, me, sc: (0, j))

    s1 = pl.BlockSpec((r, cb), lambda j, me, sc: (0, j * NK + k))
    s2 = pl.BlockSpec((rb, dc), lambda j, me, sc: (k, j))
    specs = ([col(q) for q in range(n)] + [straight()] * n
             + [s1] * 4 + [s2] * 4)
    args = [p1] + got1 + [p2] + got2 + st1 + st2
    alias = {}
    if prev is not None:
        alias = {2 + len(args) + i: i for i in range(6)}
        specs = specs + [pl.BlockSpec(memory_space=pl.ANY)] * 6
        args = args + prev
    specs = specs + [LATER] * len(after)
    args = args + after
    out = pl.pallas_call(
        functools.partial(adam_kernel, n),
        grid_spec=pltpu.PrefetchScalarGridSpec(
            num_scalar_prefetch=2, grid=(n,), in_specs=specs,
            out_specs=[s1] * 3 + [s2] * 3 + [pl.BlockSpec((r + rb, cb), lambda j, me, sc: (0, j))]),
        out_shape=[jax.ShapeDtypeStruct((r, ff), f32)] * 3
        + [jax.ShapeDtypeStruct((f, d), f32)] * 3 + [jax.ShapeDtypeStruct((r + rb, d), bf)],
        input_output_aliases=alias,
        cost_estimate=cost(r * d * 60, r * d * 76),
        name="adam", compiler_params=params())(me, sc, *args)
    return list(out[:6]), out[6]


def solution(mesh):
    n = mesh.shape['fsdp']
    tok4 = P(None, ('mp', 'fsdp'), None, None)
    tok3 = P(('mp', 'fsdp'), None, None)
    rows = P(None, ('mp', 'fsdp'), None)

    def hop(a, r):
        return lax.ppermute(a, 'fsdp', [(i, i ^ r) for i in range(n)])

    def gather(c):
        far = hop(c, 2)
        own = hop(c, 1)
        near = hop(far, 1)
        return [c, own, far, near]

    def body(x, dy, xn, w1, w2, g1, g2, m1, m2, v1, v2, hp, step):
        _, b, t, d = x.shape
        ds = d // n
        tf = step[0].astype(f32)
        me = lax.axis_index('fsdp')
        mev = me.astype(jnp.int32).reshape(1)
        gy = dy.reshape(b * t, d)
        sc = jnp.stack([hp[0], hp[1], hp[2], hp[3], hp[4],
                        1.0 - hp[1] ** tf, 1.0 - hp[2] ** tf, hp[0]])

        xl = x.reshape(b * t, d)
        xc = xn.reshape(b * t, d)
        cs = [gather(cast_chunk(w1[0], w2[0], k, n))
              for k in range(NK)]
        st1 = [w1[0], g1[0], m1[0], v1[0]]
        st2 = [w2[0], g2[0], m2[0], v2[0]]
        parts = [None] * NK

        def back(k, after):
            a, dh = hid(mev, xl, gy, cs[k], after)
            p2 = jnp.einsum('nf,nd->fd', a, gy, preferred_element_type=f32).astype(bf)
            p1 = jnp.einsum('nd,nf->df', xl, dh, preferred_element_type=f32).astype(bf)
            s2 = [p2[r * ds:(r + 1) * ds] for r in range(1, n)]
            s1 = [lax.dynamic_slice_in_dim(p1, (me ^ r) * ds, ds, 0) for r in range(1, n)]
            r2 = [hop(q, r) for r, q in enumerate(s2, 1)]
            r1 = [hop(q, r) for r, q in enumerate(s1, 1)]
            parts[k] = p1, r1, p2, r2
            return s1 + s2

        def step_of(k, prev, after):
            prev, c = adam(mev, sc, *parts[k], st1, st2, prev, k, after)
            return prev, [c], gather(c)

        def ahead(k, full, acc, after):
            a = up(mev, xc, full, after)
            return down(a, acc, full, bf if k == NK - 1 else f32)

        full = [None] * NK
        later = back(0, [])
        later = back(1, later)
        later = back(2, later)
        prev, later, full[0] = step_of(0, None, later)
        prev, later, full[1] = step_of(1, prev, later)
        later = back(3, later)
        prev, later, full[2] = step_of(2, prev, later)
        acc = ahead(0, full[0], xc, later)
        acc = ahead(1, full[1], acc, [])
        prev, later, full[3] = step_of(3, prev, [acc])
        acc = ahead(2, full[2], acc, later)
        acc = ahead(3, full[3], acc, [acc])
        w1n, m1n, v1n, w2n, m2n, v2n = prev
        return (w1n[None], w2n[None], m1n[None], m2n[None], v1n[None], v2n[None],
                acc.reshape(b, t, d))

    return jax.shard_map(body, mesh=mesh,
                         in_specs=(tok4, tok3, tok3) + (rows,) * 8 + (P(), P()),
                         out_specs=(rows,) * 6 + (tok3,), check_vma=False)
```

```python
import functools

import jax
import jax.numpy as jnp
from jax import lax
from jax.experimental import pallas as pl
from jax.experimental.pallas import tpu as pltpu
from jax.sharding import PartitionSpec as P


NK = 4
TM = 512
TN = 512
C0 = 0.7978845608028654
C1 = 0.044715
f32 = jnp.float32
bf = jnp.bfloat16
VMEM = 60 * 1024 * 1024
LATER = pl.BlockSpec(memory_space=pl.ANY)


def params(n=1):
    return pltpu.CompilerParams(vmem_limit_bytes=VMEM, dimension_semantics=("arbitrary",) * n)


def whole(shape, row=0):
    return pl.BlockSpec(shape, lambda *_: (row, 0), pipeline_mode=pl.Buffered(1))


def cost(flops, nbytes):
    return pl.CostEstimate(flops=flops, bytes_accessed=nbytes, transcendentals=0)


def cast_kernel(w1, w2, out):
    r = w1.shape[0]
    out[:r] = w1[...].astype(bf)
    out[r:] = w2[...].astype(bf)


def cast_chunk(w1, w2, k, n):
    r, cb = w1.shape[0], w1.shape[1] // (n * NK)
    d = w2.shape[1]
    rb, dc = w2.shape[0] // NK, d // n
    return pl.pallas_call(
        cast_kernel, grid=(n,),
        in_specs=[pl.BlockSpec((r, cb), lambda j: (0, j * NK + k)),
                  pl.BlockSpec((rb, dc), lambda j: (k, j))],
        out_specs=pl.BlockSpec((r + rb, cb), lambda j: (0, j)),
        out_shape=jax.ShapeDtypeStruct((r + rb, d), bf),
        cost_estimate=cost(r * d * 2, r * d * 12),
        name="cast_chunk", compiler_params=params())(w1, w2)


def join1(me, cs, n, w1, qs):
    b = cs[0].shape[0]
    w = w1.shape[1] // n
    for q, c in zip(qs, cs):
        i = pl.multiple_of(((me ^ q) % len(qs)) * b, 128)
        for r in range(n):
            j = pl.multiple_of((me ^ r) * w, 128)
            w1[pl.ds(i, b), r * w:(r + 1) * w] = c[:, pl.ds(j, w)]


def join2(cs, n, w2):
    b = cs[0].shape[0]
    for q in range(n):
        w2[q * b:(q + 1) * b, :] = cs[q][...]


def hid_kernel(n, me, x, dy, *refs):
    c1, c2 = refs[:n], refs[n:2 * n]
    a_out, dh_out, w1, w2 = refs[-4:]

    @pl.when(pl.program_id(0) == 0)
    def _():
        join1(me[0], c1, n, w1, range(n))
        join2(c2, n, w2)

    xv = x[...]
    dv = dy[...]
    for s in range(0, w1.shape[1], TN):
        h = jnp.dot(xv, w1[:, s:s + TN], preferred_element_type=f32)
        da = lax.dot_general(dv, w2[s:s + TN, :], (((1,), (1,)), ((), ())),
                             preferred_element_type=f32)
        hh = h * h
        t = jnp.tanh(h * (C0 + (C0 * C1) * hh))
        p = 0.5 + 0.5 * t
        a_out[:, s:s + TN] = (h * p).astype(bf)
        gp = p + (0.5 * h) * (1.0 - t * t) * (C0 + (3.0 * C0 * C1) * hh)
        dh_out[:, s:s + TN] = (da * gp).astype(bf)


def hid(me, x, dy, cs, after):
    n = len(cs)
    t, d = x.shape
    h2, w = cs[0].shape
    hh = h2 // 2
    tok = pl.BlockSpec((TM, d), lambda i, *_: (i, 0))
    return pl.pallas_call(
        functools.partial(hid_kernel, n),
        grid_spec=pltpu.PrefetchScalarGridSpec(
            num_scalar_prefetch=1, grid=(t // TM,),
            in_specs=[tok, tok] + [whole((hh, w))] * n + [whole((hh, w), 1)] * n + [LATER] * len(after),
            out_specs=[pl.BlockSpec((TM, w), lambda i, *_: (i, 0))] * 2,
            scratch_shapes=[pltpu.VMEM((n * hh, w), bf), pltpu.VMEM((n * hh, d), bf)]),
        out_shape=[jax.ShapeDtypeStruct((t, w), bf)] * 2,
        cost_estimate=cost(4 * t * d * w, 8 * t * d),
        name="hid", compiler_params=params())(me, x, dy, *cs, *cs, *after)


def up_kernel(n, qs, me, x, *refs):
    c1 = refs[:len(qs)]
    a_out, w1 = refs[-2:]
    part = refs[len(qs)] if qs[0] else None

    @pl.when(pl.program_id(0) == 0)
    def _():
        join1(me[0], c1, n, w1, qs)

    xv = x[...]
    for s in range(0, w1.shape[1], TN):
        h = jnp.dot(xv, w1[:, s:s + TN], preferred_element_type=f32)
        if part is not None:
            h = part[:, s:s + TN] + h
        if a_out.dtype == f32:
            a_out[:, s:s + TN] = h
        else:
            t = jnp.tanh(h * (C0 + (C0 * C1) * (h * h)))
            a_out[:, s:s + TN] = (h * (0.5 + 0.5 * t)).astype(bf)


def up(me, x, cs, n, qs, part, after):
    t, d = x.shape
    hh = d // n
    w = cs[0].shape[1]
    half = len(qs) // 2 if len(qs) < n else 0
    dk = d * len(qs) // n
    side = pl.BlockSpec((TM, dk), lambda i, me: (i, ((me[0] ^ qs[0]) // len(qs))))
    tok = pl.BlockSpec((TM, w), lambda i, *_: (i, 0))
    extra = [] if part is None else [part]
    return pl.pallas_call(
        functools.partial(up_kernel, n, qs),
        grid_spec=pltpu.PrefetchScalarGridSpec(
            num_scalar_prefetch=1, grid=(t // TM,),
            in_specs=[side] + [whole((hh, w))] * len(qs) + [tok] * len(extra) + [LATER] * len(after),
            out_specs=tok,
            scratch_shapes=[pltpu.VMEM((dk, w), bf)]),
        out_shape=jax.ShapeDtypeStruct((t, w), f32 if half and part is None else bf),
        cost_estimate=cost(2 * t * dk * w, 4 * t * d),
        name="up", compiler_params=params())(me, x, *cs, *extra, *after)


def down_kernel(n, a, acc, *refs):
    c2 = refs[:n]
    out, w2 = refs[-2:]

    @pl.when(pl.program_id(0) == 0)
    def _():
        join2(c2, n, w2)

    av = a[...]
    for s in range(0, w2.shape[1], TN):
        o = jnp.dot(av, w2[:, s:s + TN], preferred_element_type=f32)
        out[:, s:s + TN] = (acc[:, s:s + TN].astype(f32) + o).astype(out.dtype)


def down(a, acc, cs, row, side, dtype):
    n = len(cs)
    t, d = acc.shape
    hh = cs[0].shape[0] // (row + 1)
    tok = pl.BlockSpec((TM, d), lambda i: (i, 0))
    return pl.pallas_call(
        functools.partial(down_kernel, n), grid=(t // TM,),
        in_specs=[pl.BlockSpec((TM, n * hh), lambda i: (i, side)), tok] + [whole((hh, d), row)] * n,
        out_specs=tok,
        scratch_shapes=[pltpu.VMEM((n * hh, d), bf)],
        out_shape=jax.ShapeDtypeStruct((t, d), dtype),
        cost_estimate=cost(2 * t * d * n * hh, 10 * t * d),
        name="down", compiler_params=params())(a, acc, *cs)


def adam_kernel(n, halves, me, sc, *refs):
    lr, b1, b2, eps, wd, u1, u2 = (sc[i] for i in range(7))
    outs = refs[-3 * halves - 1:]
    b = outs[-1].shape[0] // halves
    for half in range(halves):
        ps = refs[half * n:(half + 1) * n]
        w, ga, m, v = (refs[halves * n + half * 4 + i][...] for i in range(4))
        s = ps[0][...].astype(f32)
        for q in range(1, n):
            s = s + ps[q][...].astype(f32)
        g = (ga + s) / 2.0
        mn = b1 * m + (1.0 - b1) * g
        vn = b2 * v + (1.0 - b2) * g * g
        upd = (mn / u1) / (jnp.sqrt(vn / u2) + eps)
        wn = w - lr * (upd + wd * w)
        outs[half * 3][...] = wn
        outs[half * 3 + 1][...] = mn
        outs[half * 3 + 2][...] = vn
        outs[-1][half * b:(half + 1) * b, :] = wn.astype(bf)


def adam(me, sc, n, k, jobs, after):
    specs, args, states, state_specs, outs, out_specs, done = [], [], [], [], [], [], []
    rows = 0
    for which, ps, st, prev in jobs:
        r, c = st[0].shape
        if which == 1:
            rb, cb = r, c // (n * NK)
            spec = pl.BlockSpec((rb, cb), lambda j, me, sc: (0, j * NK + k))
            specs += [pl.BlockSpec((rb, cb), lambda j, me, sc, q=q: (0 if q else me[0], me[0] ^ q ^ j))
                      for q in range(n)]
        else:
            rb, cb = r // NK, c // n
            spec = pl.BlockSpec((rb, cb), lambda j, me, sc: (k, j))
            specs += [pl.BlockSpec((rb, cb), lambda j, me, sc: (0, j))] * n
        args += ps
        states += st
        state_specs += [spec] * 4
        outs += [jax.ShapeDtypeStruct((r, c), f32)] * 3
        out_specs += [spec] * 3
        done += prev or []
        rows += rb
    args += states
    alias = {2 + len(args) + i: i for i in range(len(done))}
    args += done + after
    specs += state_specs + [LATER] * (len(done) + len(after))
    out = pl.pallas_call(
        functools.partial(adam_kernel, n, len(jobs)),
        grid_spec=pltpu.PrefetchScalarGridSpec(
            num_scalar_prefetch=2, grid=(n,), in_specs=specs,
            out_specs=out_specs + [pl.BlockSpec((rows, cb), lambda j, me, sc: (0, j))]),
        out_shape=outs + [jax.ShapeDtypeStruct((rows, n * cb), bf)],
        input_output_aliases=alias,
        cost_estimate=cost(rows * n * cb * 30, rows * n * cb * 38),
        name="adam", compiler_params=params())(me, sc, *args)
    return [list(out[3 * i:3 * i + 3]) for i in range(len(jobs))], out[-1]


def solution(mesh):
    n = mesh.shape['fsdp']
    tok4 = P(None, ('mp', 'fsdp'), None, None)
    tok3 = P(('mp', 'fsdp'), None, None)
    rows = P(None, ('mp', 'fsdp'), None)

    def hop(a, r):
        return lax.ppermute(a, 'fsdp', [(i, i ^ r) for i in range(n)])

    def gather(c):
        far = hop(c, 2)
        own = hop(c, 1)
        near = hop(far, 1)
        return [c, own, far, near]

    def body(x, dy, xn, w1, w2, g1, g2, m1, m2, v1, v2, hp, step):
        _, b, t, d = x.shape
        ds = d // n
        tf = step[0].astype(f32)
        me = lax.axis_index('fsdp')
        mev = me.astype(jnp.int32).reshape(1)
        gy = dy.reshape(b * t, d)
        sc = jnp.stack([hp[0], hp[1], hp[2], hp[3], hp[4],
                        1.0 - hp[1] ** tf, 1.0 - hp[2] ** tf, hp[0]])

        xl = x.reshape(b * t, d)
        xc = xn.reshape(b * t, d)
        cs = [gather(cast_chunk(w1[0], w2[0], k, n))
              for k in range(NK)]
        st1 = [w1[0], g1[0], m1[0], v1[0]]
        st2 = [w2[0], g2[0], m2[0], v2[0]]
        parts = [None] * NK

        def back(k, after):
            a, dh = hid(mev, xl, gy, cs[k], after)
            p2 = jnp.einsum('nf,nd->fd', a, gy, preferred_element_type=f32).astype(bf)
            p1 = jnp.einsum('nd,nf->df', xl, dh, preferred_element_type=f32).astype(bf)
            s2 = [p2[r * ds:(r + 1) * ds] for r in range(1, n)]
            s1 = [lax.dynamic_slice_in_dim(p1, (me ^ r) * ds, ds, 0) for r in range(1, n)]
            r2 = [hop(q, r) for r, q in enumerate(s2, 1)]
            r1 = [hop(q, r) for r, q in enumerate(s1, 1)]
            parts[k] = p1, r1, p2, r2
            return s1 + s2

        def job(which, k, prev):
            p1, r1, p2, r2 = parts[k]
            return (1, [p1] + r1, st1, prev) if which == 1 else (2, [p2] + r2, st2, prev)

        def step_of(k, prev, after):
            prev, c = adam(mev, sc, n, k,
                             [job(1, k, prev[0]), job(2, k, prev[1])], after)
            return prev, [c], gather(c)

        def ahead(full, acc, after):
            a = up(mev, xc, full, n, range(n), None, after)
            return down(a, acc, full, 1, 0, f32)

        full = [None] * NK
        later = back(0, [])
        later = back(1, later)
        later = back(2, later)
        prev, later, full[0] = step_of(0, [None, None], later)
        prev, later, full[1] = step_of(1, prev, later)
        later = back(3, later)
        prev, later, full[2] = step_of(2, prev, later)
        acc = ahead(full[0], xc, later)
        acc = ahead(full[1], acc, [])
        acc = ahead(full[2], acc, [])
        (n1,), c1 = adam(mev, sc, n, 3, [job(1, 3, prev[0])], [acc])
        f1 = gather(c1)
        half = up(mev, xc, f1[:2], n, (0, 1), None, [])
        (n2,), c2 = adam(mev, sc, n, 3, [job(2, 3, prev[1])], [half])
        f2 = gather(c2)
        a = up(mev, xc, f1[2:], n, (2, 3), half, [c2])
        acc = down(a, acc, f2[:2], 0, 0, f32)
        acc = down(a, acc, f2[2:], 0, 1, bf)
        w1n, m1n, v1n = n1
        w2n, m2n, v2n = n2
        return (w1n[None], w2n[None], m1n[None], m2n[None], v1n[None], v2n[None],
                acc.reshape(b, t, d))

    return jax.shard_map(body, mesh=mesh,
                         in_specs=(tok4, tok3, tok3) + (rows,) * 8 + (P(), P()),
                         out_specs=(rows,) * 6 + (tok3,), check_vma=False)
```
